256 devices in a mesh: team: 8 (over x, core), row: 2 (over z_hi), col: 16 (over y, z_lo).
Axes of the slice: x: 4, y: 4, z: 8 (z_hi: 2, z_lo: 4; z = z_hi * 4 + z_lo), core: 2. Of those that a mesh axis runs over, the one named last changes fastest.
Arguments:
- old_tiles: bfloat16 [8, 768, 256, 256], P('team', ('row', 'col')), may hold values from -4 to 4
- remap: int32 [8, 768], P('team', ('row', 'col')), may hold values from 0 to 255, as said below
- pivot_cols: bfloat16 [8, 5120, 1024], P('team', ('row', 'col')), may hold values from -6 to 6
- pivot_order: int32 [8, 2, 512], P('team'), may hold values from 0 to 511, each once within a row
- pivot_pattern: int32 [8, 2, 256], P('team'), may hold values 0 or 1
- block_inverses: float32 [8, 2, 3, 256], P('team'), may hold values from -0.05 to 0.05
- delays: int32 [8, 2], P('team'), may hold values from 0 to 128
Outputs:
- parent: float32 [2, 2048, 4096], P('row', 'team', 'col')
- second_panel: float32 [8, 5120, 512], P('team', ('row', 'col'))
The draws below stay inside these ranges and needn't reach their ends.
Inputs may be any that keep to these rules, and one draw needn't show every extreme that they name: `remap`: tiles that one device holds go to at most 12 distinct owners, the owner of tile (i, j) being the device at row i // 8, column j; at most 2 of one device's tiles go to one owner, and in every front some owner receives exactly 2 tiles from every device.
All inputs are finite; a program needn't handle non-finite values. No bound on the sum of `pivot_pattern` on one device may be relied on, other than what follows from the above.
Results may differ from the reference program's by a relative error of at most 0.0003.
Values may be sent and summed in bfloat16 or wider, within the bound.
A program may use at most 128 MiB of HBM per device.

```python
import jax
import jax.numpy as jnp
from jax import lax

TILE = 256
PANEL = 512
NF = 5120
OLD_DEV = 24
NC = 4096
NCT = 16
TEAMS = 8
OLD_TILES = 768
HOLD = 12
TRD = 8
TCD = 1
N_ROW = 2
N_COL = 16


def draw_remap(key, part):
    peers = N_ROW * N_COL

    def one_team(team_key):
        key_busy, key_perm, key_slot = jax.random.split(team_key, 3)
        busiest = jax.random.randint(key_busy, (), 0, peers)

        def sender_order(sender_key):
            rest = jax.random.permutation(sender_key, peers - 1) + 1
            return jnp.concatenate([jnp.zeros((1,), jnp.int32), rest.astype(jnp.int32)])
        offsets = jax.vmap(sender_order)(jax.random.split(key_perm, peers))
        chosen = offsets[:, jnp.arange(OLD_DEV, dtype=jnp.int32) % HOLD]
        owners = (busiest + chosen) % peers
        slots = jax.random.randint(key_slot, (peers, OLD_DEV), 0, TRD * TCD)
        owner_row = owners // N_COL
        owner_col = owners % N_COL
        tile_row = owner_row * TRD + slots // TCD
        tile_col = owner_col * TCD + slots % TCD
        return (tile_row * NCT + tile_col).reshape(peers * OLD_DEV).astype(jnp.int32)
    return jax.vmap(one_team)(jax.random.split(jax.random.fold_in(key, 7), TEAMS))


def touch_ends(values, stream_key, least, largest):
    longest = values.shape.index(max(values.shape))
    spots = []
    for shift in (0, 1):
        where = [jax.random.randint(jax.random.fold_in(stream_key, axis), (), 0, length) for axis, length in enumerate(values.shape)]
        where[longest] = (where[longest] + shift) % values.shape[longest]
        spots.append(tuple(where))
    return values.at[spots[0]].set(least).at[spots[1]].set(largest)


def block_levels(rng, shape, cuts, low, top_value):
    factor_of = 1.0
    for dim, shards_of in cuts:
        draws = jax.random.uniform(jax.random.fold_in(jax.random.fold_in(rng, 6), dim), (shards_of,), jnp.float32, low / len(cuts), top_value / len(cuts))
        factor_of = factor_of * jnp.repeat(jnp.exp(draws), shape[dim] // shards_of).reshape((-1,) + (1,) * (len(shape) - 1 - dim))
    return factor_of


def gaussian(key, dims, width, limit, cuts=(), kind=jnp.bfloat16):
    loudness = block_levels(key, dims, cuts, -0.22, 0.18) if cuts else 1.0
    entries = jax.random.normal(key, dims, jnp.float32) * width * loudness
    return jnp.minimum(jnp.maximum(entries, -limit), limit).astype(kind)


def setup_inputs(seed: int = 0) -> dict:
    keys = jax.random.split(jax.random.key(seed), 8)
    return {
        "old_tiles": gaussian(keys[0], (TEAMS, OLD_TILES, TILE, TILE), 0.6, 4.0, ((0, 8), (1, 32))),
        "remap": draw_remap(jax.random.fold_in(keys[7], 71), 0),
        "pivot_cols": gaussian(keys[2], (TEAMS, NF, 2 * PANEL), 1.0, 6.0, ((0, 8), (1, 32))),
        "pivot_order": jax.vmap(lambda own: jax.random.permutation(own, PANEL))(jax.random.split(keys[3], TEAMS * 2)).reshape((TEAMS, 2, PANEL)).astype(jnp.int32),
        "pivot_pattern": touch_ends((jax.random.randint(keys[4], (TEAMS, 2, PANEL // 2), 0, 2) < 1).astype(jnp.int32), jax.random.fold_in(keys[4], 1), 0, 1),
        "block_inverses": gaussian(keys[5], (TEAMS, 2, 3, PANEL // 2), 0.02, 0.05, ((0, 8),), jnp.float32),
        "delays": touch_ends(jax.random.randint(keys[6], (TEAMS, 2), 0, PANEL // 4 + 1), jax.random.fold_in(keys[6], 1), 0, (PANEL // 4 + 1) - 1).astype(jnp.int32),
    }


def make_coeffs(inverses, pattern, delay):
    half_panel = PANEL // 2
    positions = jnp.arange(PANEL, dtype=jnp.int32)
    active = (positions < PANEL - delay).astype(jnp.float32)
    active_lo = active[:half_panel]
    active_hi = active[half_panel:]
    diag_one = inverses[0] * active_lo
    off_diag = inverses[1] * pattern.astype(jnp.float32) * active_lo * active_hi
    diag_two = inverses[2] * active_hi
    return diag_one, off_diag, diag_two


def scale_pivots(columns, coeffs):
    diag_one, off_diag, diag_two = coeffs
    half_panel = PANEL // 2
    left_half = columns[:, :half_panel]
    right_half = columns[:, half_panel:]
    return jnp.concatenate([left_half * diag_one + right_half * off_diag, left_half * off_diag + right_half * diag_two], axis=1)


def one_front(old_tiles, remap, pivot_cols, pivot_order, pivot_pattern, block_inverses, delays):
    old_flat = old_tiles.astype(jnp.float32).reshape(OLD_TILES, TILE * TILE)
    summed = jax.ops.segment_sum(old_flat, remap, num_segments=NCT * NCT)
    front_c = summed.reshape(NCT, NCT, TILE, TILE).transpose(0, 2, 1, 3).reshape(NC, NC)
    widened = pivot_cols.astype(jnp.float32)
    first = jnp.take(widened[:, :PANEL], pivot_order[0], axis=1)
    scaled_one = scale_pivots(first, make_coeffs(block_inverses[0], pivot_pattern[0], delays[0]))
    picked = jnp.take(first, PANEL + pivot_order[1], axis=0)
    second = jnp.take(widened[:, PANEL:], pivot_order[1], axis=1) - jnp.dot(scaled_one, picked.T, precision=lax.Precision.HIGHEST, preferred_element_type=jnp.float32)
    scaled_two = scale_pivots(second, make_coeffs(block_inverses[1], pivot_pattern[1], delays[1]))
    pivot_span = 2 * PANEL
    result = front_c - jnp.dot(scaled_one[pivot_span:], first[pivot_span:].T, precision=lax.Precision.HIGHEST, preferred_element_type=jnp.float32)
    result = result - jnp.dot(scaled_two[pivot_span:], second[pivot_span:].T, precision=lax.Precision.HIGHEST, preferred_element_type=jnp.float32)
    return result, second


def reference(old_tiles, remap, pivot_cols, pivot_order, pivot_pattern, block_inverses, delays):
    def advance(total, inputs):
        result, second = one_front(*inputs)
        return total + result, second

    total, seconds = lax.scan(advance, jnp.zeros((NC, NC), jnp.float32), (old_tiles, remap, pivot_cols, pivot_order, pivot_pattern, block_inverses, delays))
    return total.reshape(N_ROW, NC // N_ROW, NC), seconds
```

```python
import jax
import jax.numpy as jnp
from jax import lax
from jax.experimental import pallas as pl
from jax.experimental.pallas import tpu as pltpu
from jax.sharding import Mesh
from jax.sharding import PartitionSpec as P

AXES = ("x", "core", "zh", "y", "zl")
ID = pl.DeviceIdType.MESH
HALF = 256
PANEL = 512
TILE = 256
SHARD = 160
PIVOTS = 1024
F32 = jnp.float32
BF16 = jnp.bfloat16
VMEM = pl.BlockSpec(memory_space=pltpu.VMEM)


def place():
    x = lax.axis_index("x")
    core = lax.axis_index("core")
    z = lax.axis_index("zh") * 4 + lax.axis_index("zl")
    y = lax.axis_index("y")
    return x, core, y, z


def device(x, core, y, z):
    return {"x": x, "core": core, "zh": z // 4, "y": y, "zl": z % 4}


def plane_peers(x, core, y):
    peers = []
    for dx in range(4):
        for dy in range(4):
            for dc in range(2):
                if dx or dy or dc:
                    peers.append(((x + dx) % 4, (core + dc) % 2, (y + dy) % 4))
    return peers


def line_peers(x, core, y, z):
    peers = []
    for dx in range(4):
        for dc in range(2):
            if dx or dc:
                peers.append((0, device((x + dx) % 4, (core + dc) % 2, y, z)))
    for dy in range(1, 4):
        peers.append((1, device(x, core, (y + dy) % 4, z)))
    for dz in range(1, 8):
        peers.append((2, device(x, core, y, (z + dz) % 8)))
    return peers


def enter_all(x, core, y, z, gate):
    barrier = pltpu.get_barrier_semaphore()
    peers = line_peers(x, core, y, z)
    for _, peer in peers:
        pl.semaphore_signal(barrier, inc=1, device_id=peer, device_id_type=ID)
    pl.semaphore_wait(barrier, len(peers))
    for axis in (1, 2):
        group = [peer for kind, peer in peers if kind == axis]
        for peer in group:
            pl.semaphore_signal(gate.at[axis - 1], inc=1, device_id=peer, device_id_type=ID)
        pl.semaphore_wait(gate.at[axis - 1], len(group))


def send(src, dst, send_sem, recv_sem, peer):
    copy = pltpu.make_async_remote_copy(
        src_ref=src, dst_ref=dst, send_sem=send_sem, recv_sem=recv_sem, device_id=peer, device_id_type=ID
    )
    copy.start()
    return copy


def wait_bytes(ref, sem):
    pltpu.make_async_copy(ref, ref, sem).wait()


def exchange_kernel(
    tiles, tags, shard, zrows, yrows, grows, trecv, tagrecv,
    zu_s, zu_r, zd_s, zd_r, y_s, y_r, gu_s, gu_r, gd_s, gd_r, t_s, t_r, gate,
):
    x, core, y, z = place()
    enter_all(x, core, y, z, gate)
    up = device(x, core, y, (z + 1) % 8)
    down = device(x, core, y, (z + 7) % 8)
    right = device(x, core, (y + 1) % 4, z)
    left = device(x, core, (y + 3) % 4, z)
    mine = (x * 2 + core) * 4 + y
    half = SHARD // 2
    sent = []
    sent.append(send(shard, yrows.at[y], y_s.at[0], y_r.at[0], right))
    sent.append(send(shard, yrows.at[y], y_s.at[1], y_r.at[1], left))
    sent.append(send(shard, zrows.at[z], zu_s.at[0], zu_r.at[0], up))
    sent.append(send(shard, zrows.at[z], zd_s.at[0], zd_r.at[0], down))
    for px, pc, py in plane_peers(x, core, y):
        other = (px * 2 + pc) * 4 + py
        peer = device(px, pc, py, z)
        send(tags, tagrecv.at[mine], t_s.at[1], t_r.at[1], peer)
        send(tiles.at[:, pl.ds(pl.multiple_of(other * 8, 8), 8), :], trecv.at[mine], t_s.at[0], t_r.at[0], peer)
    zrows[z] = shard[...]
    yrows[y] = shard[...]
    tagrecv[mine] = tags[...]
    trecv[mine] = tiles[:, pl.ds(pl.multiple_of(mine * 8, 8), 8), :]

    def land(ref, sem):
        wait_bytes(ref, sem)

    y_left = (y + 3) % 4
    y_right = (y + 1) % 4
    land(yrows.at[y_left], y_r.at[0])
    part = yrows.at[y_left, 0:half]
    sent.append(send(part, part, y_s.at[2], y_r.at[2], right))
    land(yrows.at[y_right], y_r.at[1])
    part = yrows.at[y_right, half:SHARD]
    sent.append(send(part, part, y_s.at[3], y_r.at[3], left))
    for step in range(2, 5):
        src = (z + 9 - step) % 8
        land(zrows.at[src], zu_r.at[step - 2])
        part = zrows.at[src] if step < 4 else zrows.at[src, 0:half]
        sent.append(send(part, part, zu_s.at[step - 1], zu_r.at[step - 1], up))
        src = (z + step - 1) % 8
        land(zrows.at[src], zd_r.at[step - 2])
        part = zrows.at[src] if step < 4 else zrows.at[src, half:SHARD]
        sent.append(send(part, part, zd_s.at[step - 1], zd_r.at[step - 1], down))
        if step == 2:
            opposite = (y + 2) % 4
            land(yrows.at[opposite, 0:half], y_r.at[2])
            land(yrows.at[opposite, half:SHARD], y_r.at[3])
            pivot_y = jnp.where(z == 3, 0, 1)

            @pl.when(z < 4)
            def _():
                grows[z] = yrows[pivot_y, :, 0:PANEL]
                first = yrows.at[pivot_y, :, 0:PANEL]
                send(first, grows.at[z], gu_s.at[0], gu_r.at[0], up)
                send(first, grows.at[z], gd_s.at[0], gd_r.at[0], down)

    for step in range(2, 5):
        src = (z + 9 - step) % 8

        @pl.when(src < 4)
        def _(step=step, src=src):
            land(grows.at[src], gu_r.at[step - 2])
            send(grows.at[src], grows.at[src], gu_s.at[step - 1], gu_r.at[step - 1], up)

        src = (z + step - 1) % 8

        @pl.when(src < 4)
        def _(step=step, src=src):
            land(grows.at[src], gd_r.at[step - 2])
            if step < 4:
                send(grows.at[src], grows.at[src], gd_s.at[step - 1], gd_r.at[step - 1], down)

    @pl.when((z + 4) % 8 < 4)
    def _():
        land(grows.at[(z + 4) % 8], gu_r.at[3])

    land(zrows.at[(z + 4) % 8, 0:half], zu_r.at[3])
    land(zrows.at[(z + 4) % 8, half:SHARD], zd_r.at[3])
    land(trecv.at[0:31], t_r.at[0])
    land(tagrecv.at[0:31], t_r.at[1])
    wait_bytes(trecv.at[0:31], t_s.at[0])
    wait_bytes(tagrecv.at[0:31], t_s.at[1])
    for copy in sent:
        copy.wait_send()
    for step in range(1, 5):
        src = (z + 9 - step) % 8

        @pl.when(src < 4)
        def _(step=step, src=src):
            wait_bytes(grows.at[src], gu_s.at[step - 1])

        if step < 4:
            src = (z + step - 1) % 8

            @pl.when(src < 4)
            def _(step=step, src=src):
                wait_bytes(grows.at[src], gd_s.at[step - 1])


def exchange(tiles, tags, shard):
    held = tiles.shape[0]
    dma = pltpu.SemaphoreType.DMA
    return pl.pallas_call(
        exchange_kernel,
        out_shape=(
            jax.ShapeDtypeStruct((8, SHARD, 2 * PANEL), BF16),
            jax.ShapeDtypeStruct((4, SHARD, 2 * PANEL), BF16),
            jax.ShapeDtypeStruct((4, SHARD, PANEL), BF16),
            jax.ShapeDtypeStruct((32, held, 8, TILE), BF16),
            jax.ShapeDtypeStruct((32, 8, 128), jnp.int32),
        ),
        in_specs=[VMEM] * 3,
        out_specs=(VMEM,) * 5,
        scratch_shapes=[
            dma((4,)), dma((4,)), dma((4,)), dma((4,)), dma((4,)), dma((4,)),
            dma((4,)), dma((4,)), dma((3,)), dma((3,)), dma((2,)), dma((2,)),
            pltpu.SemaphoreType.REGULAR((2,)),
        ],
        compiler_params=pltpu.CompilerParams(collective_id=0, has_side_effects=True),
        name="exchange",
    )(tiles, tags, shard)


def scatter_kernel(index, slices, out):
    out[...] = jnp.zeros_like(out)

    @pl.loop(0, slices.shape[0], unroll=8)
    def _(k):
        out[index[k]] += slices[k].astype(F32)


def scatter(index, slices):
    return pl.pallas_call(
        scatter_kernel,
        out_shape=jax.ShapeDtypeStruct((256, 8, TILE), F32),
        in_specs=[pl.BlockSpec(memory_space=pltpu.SMEM), VMEM],
        out_specs=VMEM,
        name="scatter",
    )(index, slices)


def reduce_kernel(
    update, sums, piece, ring, cores, keep, across, up_send, up_recv, dn_send, dn_recv,
    c_s, c_r, x_s, x_r, u_s, u_r, d_s, d_r, gate,
):
    x, core, y, z = place()
    enter_all(x, core, y, z, gate)
    up = device(x, core, y, (z + 1) % 8)
    down = device(x, core, y, (z + 7) % 8)
    width = 4 * SHARD
    other = 1 - core
    sent = [
        send(
            update.at[:, pl.ds(pl.multiple_of(other * width, 128), width)],
            cores, c_s.at[0], c_r.at[0], device(x, other, y, z),
        ),
        send(sums.at[(z + 4) % 8], up_recv.at[0], u_s.at[0], u_r.at[0], up),
        send(sums.at[(z + 5) % 8], dn_recv.at[0], d_s.at[0], d_r.at[0], down),
    ]
    wait_bytes(cores, c_r.at[0])
    keep[...] = update[:, pl.ds(pl.multiple_of(core * width, 128), width)] + cores[...]
    for dx in (1, 3, 2):
        px = (x + dx) % 4
        sent.append(
            send(
                keep.at[pl.ds(pl.multiple_of(px * SHARD, 8), SHARD)],
                across.at[3 - dx], x_s.at[dx - 1], x_r.at[3 - dx], device(px, core, y, z),
            )
        )
    for step in range(1, 4):
        wait_bytes(up_recv.at[step - 1], u_r.at[step - 1])
        up_send[step - 1] = up_recv[step - 1] + sums[(z + 4 - step) % 8]
        sent.append(send(up_send.at[step - 1], up_recv.at[step], u_s.at[step], u_r.at[step], up))
        if step < 3:
            wait_bytes(dn_recv.at[step - 1], d_r.at[step - 1])
            dn_send[step - 1] = dn_recv[step - 1] + sums[(z + 5 + step) % 8]
            sent.append(send(dn_send.at[step - 1], dn_recv.at[step], d_s.at[step], d_r.at[step], down))
    for slot in range(3):
        wait_bytes(across.at[slot], x_r.at[slot])
    piece[...] = (
        keep[pl.ds(pl.multiple_of(x * SHARD, 8), SHARD)] + across[0] + across[1] + across[2]
    )
    wait_bytes(up_recv.at[3], u_r.at[3])
    wait_bytes(dn_recv.at[2], d_r.at[2])
    ring[...] = sums[z] + up_recv[3] + dn_recv[2]
    for copy in sent:
        copy.wait_send()


def reduce_both(update, sums):
    dma = pltpu.SemaphoreType.DMA
    block = (32, 8, TILE)
    return pl.pallas_call(
        reduce_kernel,
        out_shape=(
            jax.ShapeDtypeStruct((SHARD, 4 * SHARD), F32),
            jax.ShapeDtypeStruct(block, F32),
        ),
        in_specs=[VMEM] * 2,
        out_specs=(VMEM,) * 2,
        scratch_shapes=[
            pltpu.VMEM((4 * SHARD, 4 * SHARD), F32),
            pltpu.VMEM((4 * SHARD, 4 * SHARD), F32),
            pltpu.VMEM((3, SHARD, 4 * SHARD), F32),
            pltpu.VMEM((3, *block), F32),
            pltpu.VMEM((4, *block), F32),
            pltpu.VMEM((2, *block), F32),
            pltpu.VMEM((3, *block), F32),
            dma((1,)), dma((1,)), dma((3,)), dma((3,)), dma((4,)), dma((4,)), dma((3,)), dma((3,)),
            pltpu.SemaphoreType.REGULAR((2,)),
        ],
        compiler_params=pltpu.CompilerParams(collective_id=1, has_side_effects=True),
        name="reduce_both",
    )(update, sums)


def deliver_kernel(piece, ring, parent, upd, tot, p_s, p_l, p_r, t_s, t_r, gate):
    x, core, y, z = place()
    enter_all(x, core, y, z, gate)
    row0 = (z // 4) * 2560 + x * 640 + (z % 4) * SHARD - PIVOTS
    col0 = core * 2560 + y * 640 - PIVOTS

    def each(action):
        for a in range(5):
            for b in range(5):
                row = row0 + 32 * a
                col = col0 + 128 * b
                i = row // TILE
                j = col // TILE
                px, pc, pz, py = (i % 8) // 2, i % 2, (i // 8) * 4 + j % 4, j // 4
                real = (row >= 0) & (col >= 0)
                own = (px == x) & (pc == core) & (pz == z) & (py == y)
                src = piece.at[32 * a : 32 * a + 32, 128 * b : 128 * b + 128]
                dst = upd.at[
                    pl.ds(pl.multiple_of(row % TILE, 32), 32), pl.ds(pl.multiple_of(col % TILE, 128), 128)
                ]
                action(real, own, src, dst, device(px, pc, py, pz), 5 * a + b)

    def start(real, own, src, dst, peer, n):
        @pl.when(real & jnp.logical_not(own))
        def _():
            send(src, dst, p_s.at[n], p_r.at[0], peer)

        @pl.when(real & own)
        def _():
            pltpu.make_async_copy(src, dst, p_r.at[0]).start()

    def finish(real, own, src, dst, peer, n):
        @pl.when(real & jnp.logical_not(own))
        def _():
            wait_bytes(src, p_s.at[n])

    each(start)
    mine = (x * 2 + core) * 4 + y
    for px, pc, py in plane_peers(x, core, y):
        other = (px * 2 + pc) * 4 + py
        send(
            ring.at[pc * 4 + py + px * 8],
            tot.at[mine], t_s.at[0], t_r.at[0], device(px, pc, py, z),
        )
    tot[mine] = ring[mine]
    wait_bytes(upd, p_r.at[0])
    wait_bytes(tot.at[0:31], t_r.at[0])
    wait_bytes(tot.at[0:31], t_s.at[0])
    for p in range(32):
        parent[8 * p : 8 * p + 8, :] = tot[p] - upd[8 * p : 8 * p + 8, :]
    each(finish)


def deliver(piece, ring):
    dma = pltpu.SemaphoreType.DMA
    return pl.pallas_call(
        deliver_kernel,
        out_shape=jax.ShapeDtypeStruct((TILE, TILE), F32),
        in_specs=[VMEM] * 2,
        out_specs=VMEM,
        scratch_shapes=[
            pltpu.VMEM((TILE, TILE), F32),
            pltpu.VMEM((32, 8, TILE), F32),
            dma((25,)), dma((1,)), dma((1,)), dma((1,)), dma((1,)),
            pltpu.SemaphoreType.REGULAR((2,)),
        ],
        compiler_params=pltpu.CompilerParams(collective_id=2, has_side_effects=True),
        name="deliver",
    )(piece, ring)


def split(v):
    hi = lax.reduce_precision(v, 8, 7)
    return hi.astype(BF16), (v - hi).astype(BF16)


def dot(a, b, dims):
    return lax.dot_general(a, b, (dims, ((), ())), preferred_element_type=F32)


def dot2(parts, b, dims):
    return dot(parts[0], b, dims) + dot(parts[1], b, dims)


def raw_coeffs(inverses, pattern, delay, order):
    positions = jnp.arange(PANEL, dtype=jnp.int32)
    active = (positions < PANEL - delay).astype(F32)
    lo, hi = active[:HALF], active[HALF:]
    da = inverses[0] * lo
    db = inverses[1] * pattern.astype(F32) * lo * hi
    dc = inverses[2] * hi
    diag = jnp.concatenate([da, dc])
    off = jnp.concatenate([db, db])
    partner = jnp.concatenate([order[HALF:], order[:HALF]])
    lanes = jnp.arange(PANEL, dtype=jnp.int32)
    here = order[:, None] == lanes[None, :]
    diag_raw = jnp.sum(jnp.where(here, diag[:, None], 0.0), axis=0)
    off_raw = jnp.sum(jnp.where(here, off[:, None], 0.0), axis=0)
    partner_raw = jnp.sum(jnp.where(here, partner[:, None], 0), axis=0)
    swap = (lanes[:, None] == partner_raw[None, :]).astype(BF16)
    return diag_raw, off_raw, swap


ROWS = ((1,), (1,))
COLS = ((1,), (0,))


def eliminate(zrows, yrows, grows, orders, pattern, inverses, delays, y):
    d1, o1, q1 = raw_coeffs(inverses[0], pattern[0], delays[0], orders[0])
    d2, o2, q2 = raw_coeffs(inverses[1], pattern[1], delays[1], orders[1])
    g = jnp.concatenate([grows[3, 32:], grows[0], grows[1], grows[2, :64]], axis=0)
    m1 = yrows[:, :, :PANEL].reshape(4 * SHARD, PANEL)
    m2 = yrows[:, :, PANEL:].reshape(4 * SHARD, PANEL)
    n1 = zrows[:, :, :PANEL].reshape(8 * SHARD, PANEL)
    n2 = zrows[:, :, PANEL:].reshape(8 * SHARD, PANEL)
    h1 = split(g.astype(F32) * d1 + dot(g, q1, COLS) * o1)
    second = m2.astype(F32) - (dot(m1, h1[0], ROWS) + dot(m1, h1[1], ROWS))
    y2 = second * d2 + dot2(split(second), q2, COLS) * o2
    y2s = split(y2)
    back = m1.astype(F32) - dot2(y2s, g, COLS)
    w1 = back * d1 + dot2(split(back), q1, COLS) * o1
    update = dot2(split(w1), n1, ROWS) + dot2(y2s, n2, ROWS)
    own = lax.dynamic_slice_in_dim(second, y * SHARD, SHARD, 0)
    perm = (jnp.arange(PANEL, dtype=jnp.int32)[:, None] == orders[1][None, :]).astype(BF16)
    return update, dot2(split(own), perm, COLS)


def local(old_tiles, remap, pivot_cols, pivot_order, pivot_pattern, block_inverses, delays):
    y = lax.axis_index("y")
    held = old_tiles.shape[1]
    tags = jnp.zeros((8, 128), jnp.int32).at[0, :held].set(remap[0])
    zrows, yrows, grows, trecv, tagrecv = exchange(old_tiles[0], tags, pivot_cols[0])
    target = tagrecv[:, 0, :held].reshape(-1)
    i, j = target // 16, target % 16
    index = ((i // 8) * 4 + j % 4) * 32 + (i % 8) * 4 + j // 4
    sums = scatter(index, trecv.reshape(32 * held, 8, TILE))
    update, second = eliminate(
        zrows, yrows, grows, pivot_order[0], pivot_pattern[0], block_inverses[0], delays[0], y
    )
    piece, ring = reduce_both(update, sums.reshape(8, 32, 8, TILE))
    parent = deliver(piece, ring)
    return parent[None], second[None]


def solution(mesh):
    grid = Mesh(mesh.devices.reshape(4, 2, 2, 4, 4), AXES)
    team, row_col = ("x", "core"), ("zh", "y", "zl")
    in_specs = (
        P(team, row_col, None, None),
        P(team, row_col),
        P(team, row_col, None),
        P(team, None, None),
        P(team, None, None),
        P(team, None, None, None),
        P(team, None),
    )
    out_specs = (P("zh", team, ("y", "zl")), P(team, row_col, None))
    return jax.shard_map(local, mesh=grid, in_specs=in_specs, out_specs=out_specs, check_vma=False)
```
